32 devices in a mesh: chan: 4 (over z), tm: 8 (over y, x, core).
Axes of the slice: x: 2, y: 2, z: 4, core: 2. Of those that a mesh axis runs over, the one named last changes fastest.
Arguments:
- trajectory: float32 [512, 8, 4096], P('tm', None, 'chan'), may hold values from -40 to 40
- initial: float32 [8, 4096], P(None, 'chan'), may hold values from -6 to 6
- drive_gate: bfloat16 [512, 8, 4096], P('tm', None, 'chan'), may hold values from -16 to 4
- drive_candidate: bfloat16 [512, 8, 4096], P('tm', None, 'chan'), may hold values from -6 to 6
- gate_weight: bfloat16 [4096, 4096], P('chan'), may hold values from -0.0234375 to 0.0234375
- candidate_weight: bfloat16 [4096, 4096], P('chan'), may hold values from -0.09375 to 0.09375
Outputs:
- newton_states: float32 [512, 8, 4096], P('tm', None, 'chan')
- residual_norm: float32 [], replicated
The draws below stay inside these ranges and needn't reach their ends.
All inputs are finite; a program needn't handle non-finite values.
Results may differ from the reference program's by a relative error of at most 0.0016.
Values may be sent and summed in bfloat16 or wider, within the bound.
No kernel may reach another device: no remote copies, remote signals or barrier semaphores. Data moves between devices by JAX's collectives and lax.ppermute only.
A program may use at most 128 MiB of HBM per device.

```python
import jax
import jax.numpy as jnp
from jax import lax

H = 4096
BATCH = 8
TIME_STEP_COUNT = 512


def draw_trajectory(key, part):
    first_key = jax.random.fold_in(jax.random.fold_in(key, 11), 0)
    steps_frac = jnp.arange(TIME_STEP_COUNT, dtype=jnp.float32) / TIME_STEP_COUNT
    units_frac = jnp.arange(H, dtype=jnp.float32) / H
    growth = 0.5 * (4.0 ** steps_frac)[:, None, None] * (2.0 ** units_frac)[None, None, :]
    base = jnp.clip(jax.random.normal(first_key, (TIME_STEP_COUNT, BATCH, H), jnp.float32), -6.0, 6.0)
    values = base * growth
    return jnp.clip(values, -40.0, 40.0).astype(jnp.float32)


def draw_drive_gate(key, part):
    decay_random_key, jitter_random_key, spike_random_key = jax.random.split(jax.random.fold_in(key, 23), 3)
    log_rate = jax.random.uniform(decay_random_key, (H,), jnp.float32, jnp.log(1e-05), jnp.log(0.05))
    noise = 0.5 * jnp.clip(jax.random.normal(jitter_random_key, (TIME_STEP_COUNT, BATCH, H), jnp.float32), -4.0, 4.0)
    rate = jnp.exp(log_rate)
    spike_logits = jnp.log(rate) - jnp.log(1.0 - rate)
    spike_events = jax.random.randint(spike_random_key, (4,), 0, TIME_STEP_COUNT)
    step_values = jnp.arange(TIME_STEP_COUNT)
    spike_flags = jnp.any(step_values[:, None] == spike_events[None, :], axis=1)
    drive_level = jnp.where(spike_flags[:, None, None], -0.85, spike_logits[None, None, :])
    return jnp.clip(drive_level + noise, -16.0, 4.0).astype(jnp.bfloat16)


def shard_levels(stream_key, extent, shards, smallest, largest):
    loudness = 1.0
    for dim, blocks in shards:
        heights = jax.random.uniform(jax.random.fold_in(jax.random.fold_in(stream_key, 6), dim), (blocks,), jnp.float32, smallest / len(shards), largest / len(shards))
        loudness = loudness * jnp.repeat(jnp.exp(heights), extent[dim] // blocks).reshape((-1,) + (1,) * (len(extent) - 1 - dim))
    return loudness


def gaussian(key, dims, scale, most, cuts=(), kind=jnp.bfloat16):
    gain = shard_levels(key, dims, cuts, -0.22, 0.18) if cuts else 1.0
    entries = jax.random.normal(key, dims, jnp.float32) * scale * gain
    return jnp.minimum(jnp.maximum(entries, -most), most).astype(kind)


def setup_inputs(seed: int = 0) -> dict:
    key_list = jax.random.split(jax.random.key(seed), 7)
    return {
        "trajectory": draw_trajectory(jax.random.fold_in(key_list[6], 71), 0),
        "initial": gaussian(key_list[1], (BATCH, H), 1.0, 6.0, ((1, 4),), jnp.float32),
        "drive_gate": draw_drive_gate(jax.random.fold_in(key_list[6], 71), 0),
        "drive_candidate": gaussian(key_list[3], (TIME_STEP_COUNT, BATCH, H), 1.0, 6.0, ((0, 8), (2, 4))),
        "gate_weight": gaussian(key_list[4], (H, H), (16 * H) ** -0.5, 0.0234375, ((0, 4),)),
        "candidate_weight": gaussian(key_list[5], (H, H), H ** -0.5, 0.09375, ((0, 4),)),
    }


def advance(state, inputs):
    state = inputs[0] * state + inputs[1]
    return (state, state)

def reference(trajectory, initial, drive_gate, drive_candidate, gate_weight, candidate_weight):
    previous = jnp.concatenate([initial[None], trajectory[:-1]], 0)
    flat = previous.reshape(-1, H).astype(jnp.bfloat16)
    gate_pre = jnp.dot(flat, gate_weight, preferred_element_type=jnp.float32).reshape(previous.shape) + drive_gate.astype(jnp.float32)
    candidate_pre = jnp.dot(flat, candidate_weight, preferred_element_type=jnp.float32).reshape(previous.shape) + drive_candidate.astype(jnp.float32)
    gate_diagonal = jnp.diagonal(gate_weight).astype(jnp.float32)
    candidate_diagonal = jnp.diagonal(candidate_weight).astype(jnp.float32)
    update = jax.nn.sigmoid(gate_pre)
    candidate = jnp.tanh(candidate_pre)
    mapped = (1.0 - update) * previous + update * candidate
    jacobian = 1.0 - update + update * (1.0 - update) * (candidate - previous) * gate_diagonal + update * (1.0 - candidate * candidate) * candidate_diagonal
    offset = mapped - jacobian * previous
    _, newton_states = lax.scan(advance, initial, (jacobian, offset))
    missing = trajectory - mapped
    residual_norm = jnp.sqrt(jnp.mean(missing * missing) + 1e-06)
    return (newton_states, residual_norm)
```

```python
import functools

import jax
import jax.numpy as jnp
from jax import lax
from jax.experimental import pallas as pl
from jax.experimental.pallas import tpu as pltpu
from jax.sharding import PartitionSpec as P


F32 = jnp.float32
BF16 = jnp.bfloat16
ANY = pl.BlockSpec(memory_space=pl.ANY)
SMEM = pl.BlockSpec(memory_space=pltpu.SMEM)


def swap(x, axis, mask):
    size = lax.axis_size(axis)
    return lax.ppermute(x, axis, [(i, i ^ mask) for i in range(size)])


def outer_swap(x, axis):
    size = lax.axis_size(axis)
    pairs = []
    for i in range(1, size - 1, 2):
        pairs += [(i, i + 1), (i + 1, i)]
    return lax.ppermute(x, axis, pairs)


def dot(a, b):
    return jnp.dot(a, b, preferred_element_type=F32)


def place_pieces(same_ref, other_ref, dst, time_index, sem):
    count, _, piece_rows, _ = same_ref.shape
    for j in range(count):
        for flip, ref in ((0, same_ref), (1, other_ref)):
            at = pl.multiple_of((time_index ^ (2 * j + flip)) * piece_rows, piece_rows)
            pltpu.make_async_copy(ref.at[j], dst.at[:, pl.ds(at, piece_rows), :], sem).start()


def wait_for(dst, sem):
    pltpu.make_async_copy(dst, dst, sem).wait()


def base_kernel(ids, own_rows, near_rows, gate, cand, same_ref, other_ref, sums, diagonals, weights, sems):
    width = own_rows.shape[1]
    here = pl.multiple_of(ids[0] * width, width)
    own_gate = pltpu.make_async_copy(gate.at[:, pl.ds(here, width)], weights.at[0, 0], sems.at[0])
    own_cand = pltpu.make_async_copy(cand.at[:, pl.ds(here, width)], weights.at[0, 1], sems.at[1])
    own_gate.start()
    own_cand.start()
    place_pieces(same_ref, other_ref, weights.at[1], ids[1], sems.at[2])
    own_gate.wait()
    own_cand.wait()
    step = min(128, width)
    eye = lax.broadcasted_iota(jnp.int32, (step, step), 0) == lax.broadcasted_iota(jnp.int32, (step, step), 1)
    for kind in range(2):
        for b in range(width // step):
            block = weights[0, kind, b * step : (b + 1) * step, b * step : (b + 1) * step].astype(F32)
            line = jnp.sum(jnp.where(eye, block, 0.0), axis=0, keepdims=True)
            diagonals[kind, :, b * step : (b + 1) * step] = jnp.broadcast_to(line, (8, step))
    for kind in range(2):
        sums[kind] = dot(own_rows[...], weights[0, kind])
    wait_for(weights.at[1], sems.at[2])
    for kind in range(2):
        sums[kind] += dot(near_rows[...], weights[1, kind])


def base_call(ids, own_rows, near_rows, gate, cand, same, other):
    rows, width = own_rows.shape
    return pl.pallas_call(
        base_kernel,
        in_specs=[SMEM, pl.BlockSpec(own_rows.shape), pl.BlockSpec(own_rows.shape), ANY, ANY, ANY, ANY],
        out_shape=(
            jax.ShapeDtypeStruct((2, rows, width), F32),
            jax.ShapeDtypeStruct((2, 8, width), F32),
        ),
        scratch_shapes=[pltpu.VMEM((2, 2, width, width), BF16), pltpu.SemaphoreType.DMA((3,))],
        name="base",
    )(ids, own_rows, near_rows, gate, cand, same, other)


def chunk_kernel(chunk, planes, pair_steps, ids, trajectory, before, drive_gate, drive_cand, sums, diagonals, carry, *rest):
    far = planes - 2
    near_far = rest[: 2 * pair_steps]
    pieces = rest[2 * pair_steps : 2 * pair_steps + 2 * far]
    rest = rest[2 * pair_steps + 2 * far :]
    if chunk > 0:
        rest = rest[2:]
    run_product, run_state, carry_out, weights, xs, acc, guess, sems = rest
    chan_index = ids[0]
    time_index = ids[1]
    steps = drive_gate.shape[0]
    rows = steps * 8
    fetch_sums = pltpu.make_async_copy(sums.at[:, pl.ds(chunk * rows, rows), :], acc, sems.at[2 * far])
    fetch_guess = pltpu.make_async_copy(
        trajectory.at[pl.ds(chunk * steps, steps)], guess.at[pl.ds(1, steps)], sems.at[2 * far + 1]
    )
    source = before if chunk == 0 else trajectory.at[chunk * steps - 1]
    fetch_before = pltpu.make_async_copy(source, guess.at[0], sems.at[2 * far + 2])
    pair = chan_index // 2
    odd = chan_index % 2
    for s in range(1, pair_steps + 1):
        for side in range(2):
            ref = near_far[2 * (s - 1) + side]
            from_right = (odd == 1) if side == 0 else (odd == 0)
            other_pair = jnp.where(from_right, pair + s, pair - s)
            valid = (other_pair >= 0) & (other_pair < planes // 2)
            for i in range(2):
                plane = 2 * other_pair + jnp.where(from_right, i, 1 - i)
                slot = jnp.clip((chan_index ^ plane) - 2, 0, far - 1)

                @pl.when(valid)
                def _():
                    pltpu.make_async_copy(ref.at[i], xs.at[slot], sems.at[far + slot]).start()

    for d in range(far):
        place_pieces(pieces[2 * d], pieces[2 * d + 1], weights.at[d], time_index, sems.at[d])
    fetch_sums.start()
    fetch_guess.start()
    fetch_before.start()
    fetch_sums.wait()
    for d in range(far):
        wait_for(xs.at[d], sems.at[far + d])
        wait_for(weights.at[d], sems.at[d])
        for kind in range(2):
            acc[kind] += dot(xs[d], weights[d, kind])
    fetch_guess.wait()
    fetch_before.wait()
    gate_diagonal = diagonals[0]
    cand_diagonal = diagonals[1]

    def step(t, held):
        product, state, squares = held
        at = pl.multiple_of(t * 8, 8)
        gate_pre = acc[0, pl.ds(at, 8), :] + drive_gate[t].astype(F32)
        cand_pre = acc[1, pl.ds(at, 8), :] + drive_cand[t].astype(F32)
        previous = guess[t]
        update = jax.nn.sigmoid(gate_pre)
        candidate = jnp.tanh(cand_pre)
        mapped = (1.0 - update) * previous + update * candidate
        jacobian = (
            1.0
            - update
            + update * (1.0 - update) * (candidate - previous) * gate_diagonal
            + update * (1.0 - candidate * candidate) * cand_diagonal
        )
        offset = mapped - jacobian * previous
        product = jacobian * product
        state = jacobian * state + offset
        run_product[t] = product
        run_state[t] = state
        missing = guess[t + 1] - mapped
        return product, state, squares + missing * missing

    product, state, squares = lax.fori_loop(0, steps, step, (carry[0], carry[1], carry[2]))
    carry_out[0] = product
    carry_out[1] = state
    carry_out[2] = squares


def chunk_call(chunk, chunks, ids, trajectory, before, drive_gate, drive_cand, sums, diagonals, carry, far_rows, pieces, running):
    total, batch, width = trajectory.shape
    planes = lax.axis_size("chan")
    far = planes - 2
    steps = total // chunks
    part = pl.BlockSpec((steps, batch, width), lambda g: (chunk, 0, 0))
    whole = lambda x: pl.BlockSpec(x.shape, lambda g: (0,) * x.ndim)
    operands = [ids, trajectory, before, drive_gate, drive_cand, sums, diagonals, carry, *far_rows, *pieces]
    specs = [SMEM, ANY, ANY, part, part, ANY, whole(diagonals), whole(carry)]
    specs += [ANY] * (len(far_rows) + len(pieces))
    aliases = {}
    if chunk > 0:
        aliases = {len(operands): 0, len(operands) + 1: 1}
        operands += list(running)
        specs += [ANY, ANY]
    out = pl.pallas_call(
        functools.partial(chunk_kernel, chunk, planes, planes // 2 - 1),
        grid=(1,),
        in_specs=specs,
        out_specs=(part, part, pl.BlockSpec(carry.shape, lambda g: (0, 0, 0))),
        out_shape=(
            jax.ShapeDtypeStruct(trajectory.shape, F32),
            jax.ShapeDtypeStruct(trajectory.shape, F32),
            jax.ShapeDtypeStruct(carry.shape, F32),
        ),
        input_output_aliases=aliases,
        scratch_shapes=[
            pltpu.VMEM((far, 2, width, width), BF16),
            pltpu.VMEM((far, steps * batch, width), BF16),
            pltpu.VMEM((2, steps * batch, width), F32),
            pltpu.VMEM((steps + 1, batch, width), F32),
            pltpu.SemaphoreType.DMA((2 * far + 3,)),
        ],
        name=f"chunk{chunk}",
    )(*operands)
    return out[0], out[1], out[2]


def final_kernel(ids, initial, maps, run_product, run_state, out, entry):
    @pl.when(pl.program_id(0) == 0)
    def _():
        def compose(i, state):
            return maps[i, 0] * state + maps[i, 1]

        entry[...] = lax.fori_loop(0, ids[1], compose, initial[...])

    out[...] = run_product[...] * entry[...][None] + run_state[...]


def final_call(ids, initial, maps, run_product, run_state):
    total, batch, width = run_product.shape
    steps = 8 if total % 8 == 0 else total
    part = pl.BlockSpec((steps, batch, width), lambda g: (g, 0, 0))
    return pl.pallas_call(
        final_kernel,
        grid=(total // steps,),
        in_specs=[
            SMEM,
            pl.BlockSpec(initial.shape, lambda g: (0, 0)),
            pl.BlockSpec(maps.shape, lambda g: (0, 0, 0, 0)),
            part,
            part,
        ],
        out_specs=part,
        out_shape=jax.ShapeDtypeStruct(run_product.shape, F32),
        scratch_shapes=[pltpu.VMEM(initial.shape, F32)],
        name="final",
    )(ids, initial, maps, run_product, run_state)


def local(trajectory, initial, drive_gate, drive_candidate, gate_weight, candidate_weight):
    total, batch, width = trajectory.shape
    planes = lax.axis_size("chan")
    blocks = lax.axis_size("tm")
    chan_index = lax.axis_index("chan")
    time_index = lax.axis_index("tm")
    ids = jnp.stack([chan_index, time_index]).astype(jnp.int32)
    piece_rows = width // blocks
    chunks = 4 if total % 4 == 0 else 1

    received = [None]
    for d in range(1, planes):
        column = (chan_index ^ d) * width
        piece = jnp.stack(
            [
                lax.dynamic_slice(w, (time_index * piece_rows, column), (piece_rows, width))
                for w in (gate_weight, candidate_weight)
            ]
        )
        received.append(swap(piece, "chan", d))

    arrived = lax.ppermute(trajectory[-1], "tm", [(i, i + 1) for i in range(blocks - 1)])
    before = jnp.where(time_index == 0, initial, arrived)
    own_rows = jnp.concatenate([before[None], trajectory[:-1]], 0).astype(BF16).reshape(total * batch, width)
    near_rows = swap(own_rows, "chan", 1)

    groups = []
    for d in range(1, planes):
        same = jnp.stack([received[d]] + [swap(received[d], "tm", h) for h in range(2, blocks, 2)])
        groups.append((same, swap(same, "tm", 1)))

    rows = total * batch // chunks
    far_rows = []
    for r in range(chunks):
        held = []
        payload = jnp.stack([own_rows[r * rows : (r + 1) * rows], near_rows[r * rows : (r + 1) * rows]])
        for s in range(1, planes // 2):
            outer = outer_swap(payload, "chan")
            payload = swap(outer, "chan", 1)
            held += [outer, payload]
        far_rows.append(held)

    sums, diagonals = base_call(ids, own_rows, near_rows, gate_weight, candidate_weight, *groups[0])
    pieces = [x for group in groups[1:] for x in group]
    carry = jnp.stack([jnp.ones_like(initial), jnp.zeros_like(initial), jnp.zeros_like(initial)])
    running = None
    for r in range(chunks):
        product, state, carry = chunk_call(
            r, chunks, ids, trajectory, before, drive_gate, drive_candidate, sums, diagonals, carry,
            far_rows[r], pieces, running,
        )
        running = (product, state)

    maps = lax.all_gather(carry, "tm")
    squared = jnp.sum(maps[:, 2]).reshape(1, 1)
    shares = [squared] + [swap(squared, "chan", d) for d in range(1, planes)]
    newton_states = final_call(ids, initial, maps, *running)
    squared_total = sum(shares[1:], shares[0])[0, 0]
    entries = trajectory.size * planes * blocks
    residual_norm = jnp.sqrt(squared_total / entries + 1e-06)
    return (newton_states, residual_norm)


def solution(mesh):
    placed = (
        P("tm", None, "chan"),
        P(None, "chan"),
        P("tm", None, "chan"),
        P("tm", None, "chan"),
        P("chan", None),
        P("chan", None),
    )
    return jax.shard_map(
        local, mesh=mesh, in_specs=placed, out_specs=(P("tm", None, "chan"), P()), check_vma=False
    )
```
